256 devices in a mesh: dp: 8 (over x_lo, y), mp: 32 (over z, x_hi, core).
Axes of the slice: x: 4 (x_hi: 2, x_lo: 2; x = x_hi * 2 + x_lo), y: 4, z: 8, core: 2. Of those that a mesh axis runs over, the one named last changes fastest.
Arguments:
- tokens: bfloat16 [1024, 6144], P(('dp', 'mp')), may hold values from -6 to 6
- norm_gain: float32 [6144], replicated, may hold values from 0.5 to 1.5
- w_query: bfloat16 [6144, 4096], P('dp', 'mp'), as said below
- w_key: bfloat16 [6144, 4096], P('dp', 'mp'), as said below
- w_value: bfloat16 [6144, 4096], P('dp', 'mp'), may hold values from -0.078125 to 0.078125
- w_inner: bfloat16 [6144, 24576], P('dp', 'mp'), may hold values from -0.078125 to 0.078125
- bias_inner: float32 [24576], P('mp'), may hold values from -3 to 3
- w_attn_out: bfloat16 [4096, 6144], P('mp', 'dp'), may hold values from -0.09375 to 0.09375
- w_outer: bfloat16 [24576, 6144], P('mp', 'dp'), may hold values from -0.0390625 to 0.0390625
- temper: float32 [32], P('mp'), may hold values from 0.5 to 24
Outputs:
- result: bfloat16 [1024, 6144], P(('dp', 'mp'))
The draws below stay inside these ranges and needn't reach their ends.
Inputs may be any that keep to these rules, and one draw needn't show every extreme that they name: `w_query`: entries of order 6144 ** -0.5. `w_key`: entries of order 6144 ** -0.5.
All inputs are finite; a program needn't handle non-finite values.
Results may differ from the reference program's by a relative error of at most 0.023.
Values may be sent and summed in bfloat16 or wider, within the bound.
A program may use at most 64 MiB of HBM per device.

```python
import math
import jax
import jax.numpy as jnp
from jax import lax

D = 6144
HEADS = 32
HEAD = 128
FF = 24576
HD = 4096
PATCHES = 128
TOKENS = 1024
N_DP = 8


def shared_draws(key):
    key_query = jax.random.fold_in(key, 11)
    key_noise = jax.random.fold_in(key, 12)
    key_temper = jax.random.fold_in(key, 14)
    scale = D ** (-0.5)
    limit = 6.0 * scale
    query = jnp.clip(jax.random.normal(key_query, (D, HD), jnp.float32) * scale, -limit, limit)
    noise = jnp.clip(jax.random.normal(key_noise, (D, HD), jnp.float32) * scale, -limit, limit)
    temper = jnp.exp(jax.random.uniform(key_temper, (HEADS,), jnp.float32, jnp.log(0.5), jnp.log(6.0)))
    keys = noise
    return (query, keys, temper)


def draw_w_query(key, part):
    return shared_draws(key)[0].astype(jnp.bfloat16)


def draw_w_key(key, part):
    return shared_draws(key)[1].astype(jnp.bfloat16)


def draw_temper(key, part):
    return shared_draws(key)[2]


def level_of(rng, extent, split, low, high):
    level, own = 1.0, jax.random.fold_in(rng, 6)
    for dim, blocks in split:
        heights = jnp.exp(jax.random.uniform(jax.random.fold_in(own, dim), (blocks,), jnp.float32, low / len(split), high / len(split)))
        level = level * jnp.repeat(heights, extent[dim] // blocks).reshape([-1 if axis == dim else 1 for axis in range(len(extent))])
    return level


def bell_draw(stream_key, extent, deviation, most, shards=(), kind=jnp.bfloat16):
    result = deviation * jax.random.normal(stream_key, extent, jnp.float32)
    if shards:
        result = result * level_of(stream_key, extent, shards, -0.22, 0.18)
    return jnp.clip(result, -most, most).astype(kind)


def setup_inputs(seed: int = 0) -> dict:
    streams_of = jax.random.split(jax.random.key(seed), 11)
    return {
        "tokens": bell_draw(streams_of[0], (TOKENS, D), 1.0, 6.0, ((0, 256),)),
        "norm_gain": jnp.clip(1.0 + 0.1 * jax.random.normal(streams_of[1], (D,), jnp.float32), 0.5, 1.5),
        "w_query": draw_w_query(jax.random.fold_in(streams_of[10], 71), 0),
        "w_key": draw_w_key(jax.random.fold_in(streams_of[10], 71), 0),
        "w_value": bell_draw(streams_of[4], (D, HD), D ** -0.5, 0.078125, ((0, 8), (1, 32))),
        "w_inner": bell_draw(streams_of[5], (D, FF), D ** -0.5, 0.078125, ((0, 8), (1, 32))),
        "bias_inner": bell_draw(streams_of[6], (FF,), 0.5, 3.0, ((0, 32),), jnp.float32),
        "w_attn_out": bell_draw(streams_of[7], (HD, D), HD ** -0.5, 0.09375, ((0, 32), (1, 8))),
        "w_outer": bell_draw(streams_of[8], (FF, D), FF ** -0.5, 0.0390625, ((0, 32), (1, 8))),
        "temper": draw_temper(jax.random.fold_in(streams_of[10], 71), 0),
    }


def normalize(values):
    center = values - lax.optimization_barrier(jnp.mean(values, axis=-1, keepdims=True))
    spread = lax.optimization_barrier(jnp.mean(center * center, axis=-1, keepdims=True))
    return center * lax.rsqrt(spread + 1e-06)

def reference(tokens, norm_gain, w_query, w_key, w_value, w_inner, bias_inner, w_attn_out, w_outer, temper):
    local = tokens.astype(jnp.float32)
    normed = (normalize(local) * norm_gain.astype(jnp.float32)).astype(jnp.bfloat16)
    query = jnp.dot(normed, w_query, preferred_element_type=jnp.float32).astype(jnp.bfloat16)
    keys = jnp.dot(normed, w_key, preferred_element_type=jnp.float32).astype(jnp.bfloat16)
    values = jnp.dot(normed, w_value, preferred_element_type=jnp.float32).astype(jnp.bfloat16)
    shape = (N_DP, PATCHES, HEADS, HEAD)
    query_norm = normalize(query.astype(jnp.float32).reshape(shape)).astype(jnp.bfloat16)
    key_norm = normalize(keys.astype(jnp.float32).reshape(shape)).astype(jnp.bfloat16)
    values4 = values.reshape(shape).astype(jnp.float32)
    scale = temper.astype(jnp.float32) / math.sqrt(HEAD)
    scores = jnp.einsum('bqhc,bkhc->bhqk', query_norm.astype(jnp.float32), key_norm.astype(jnp.float32))
    scores = scores * scale[None, :, None, None]
    probs = jax.nn.softmax(scores, axis=-1).astype(jnp.bfloat16)
    mixed = jnp.einsum('bhqk,bkhc->bqhc', probs.astype(jnp.float32), values4)
    mixed = mixed.astype(jnp.bfloat16).reshape(TOKENS, HD)
    inner = jnp.dot(normed, w_inner, preferred_element_type=jnp.float32) + bias_inner.astype(jnp.float32)
    activ = jax.nn.gelu(inner, approximate=False).astype(jnp.bfloat16)
    total = jnp.dot(mixed, w_attn_out, preferred_element_type=jnp.float32)
    total = total + jnp.dot(activ, w_outer, preferred_element_type=jnp.float32)
    return (local + total).astype(jnp.bfloat16)
```

```python
import math

import jax
import jax.numpy as jnp
from jax import lax
from jax.experimental import pallas as pl
from jax.experimental.pallas import tpu as pltpu
from jax.sharding import PartitionSpec as P

BF = jnp.bfloat16
F32 = jnp.float32
MESH = pl.DeviceIdType.MESH
HEAD = 128
BLK = 768
ROT = ((2, 1, 0), (1, 0, 2), (0, 2, 1))
CHUNKS = ((0, 1), (1, 3), (3, 5), (5, 7), (7, 8))
GCOLS = ((0, 384), (384, 640), (640, 896))


def first_unit(part, r):
    a, b, c = ROT[part]
    return ((r >> a) & 1) * 4 + ((r >> b) & 1) * 2 + ((r >> c) & 1)


def last_unit(part, r):
    a, b, c = ROT[part]
    return ((r >> a) & 1) + ((r >> b) & 1) * 2 + ((r >> c) & 1) * 4


def normalize(values):
    center = values - jnp.mean(values, axis=-1, keepdims=True)
    spread = jnp.mean(center * center, axis=-1, keepdims=True)
    return center * lax.rsqrt(spread + 1e-06)


def kernel(
    tok_ref, gain_ref, wq_ref, wk_ref, wv_ref, wi_ref, bias_ref, wa_ref, wo_ref, temper_ref,
    out_ref,
    w1, w2, nb, ga, xb,
    s1, r1, k1, s2, r2, k2, s3, r3, k3, yb,
    g0, g1, g2, xa, tb, d2s, d2r, zs, zr, fb, fr,
    wsem, pa_send, pa_recv, zg_send, zg_recv, dg_send, dg_recv,
    rs_send, rs_recv, ag_send, ag_recv, dr_send, dr_recv, zr_send, zr_recv, pf_send, pf_recv,
):
    dp = lax.axis_index("dp")
    mp = lax.axis_index("mp")
    xl, y = dp // 4, dp % 4
    z, q, core = mp // 4, mp % 4, mp % 2

    def near(r):
        ys = (y, y + 1 - 2 * (y % 2), 3 - y, (y + 2) % 4)[r % 4]
        return (1 - xl if r >= 4 else xl) * 4 + ys

    peers = [near(r) for r in range(8)]
    up = (z + 1 - 2 * core + 8) % 8
    down = (z - 1 + 2 * core + 8) % 8
    dev_up = (dp, up * 4 + q)
    dev_down = (dp, down * 4 + q)
    dev_pair = (dp, mp + 1 - 2 * core)
    half = pl.multiple_of(core * 64, 64)
    other = pl.multiple_of(64 - core * 64, 64)

    def send(src, dst, ssem, rsem, dev):
        pltpu.make_async_remote_copy(
            src_ref=src, dst_ref=dst, send_sem=ssem, recv_sem=rsem, device_id=dev, device_id_type=MESH
        ).start()

    def wait(ref, sem):
        pltpu.make_async_copy(ref, ref, sem).wait()

    loads = [
        pltpu.make_async_copy(wq_ref, w1.at[:, 0:128], wsem.at[0]),
        pltpu.make_async_copy(wk_ref, w1.at[:, 128:256], wsem.at[1]),
        pltpu.make_async_copy(wv_ref, w1.at[:, 256:384], wsem.at[2]),
        pltpu.make_async_copy(wi_ref, w1.at[:, 384:1152], wsem.at[3]),
        pltpu.make_async_copy(wa_ref, w2.at[0:128], wsem.at[4]),
        pltpu.make_async_copy(wo_ref, w2.at[128:896], wsem.at[5]),
    ]
    for load in loads:
        load.start()

    plane = [(r, s) for r in range(8) for s in range(4) if (r, s) != (0, 0)]
    plane_dev = {(r, s): (peers[r], z * 4 + (q + s) % 4) for r, s in plane}

    barrier = pltpu.get_barrier_semaphore()
    for key in plane:
        pl.semaphore_signal(barrier, inc=1, device_id=plane_dev[key], device_id_type=MESH)
    for dev in (dev_up, dev_down):
        pl.semaphore_signal(barrier, inc=1, device_id=dev, device_id_type=MESH)

    local = tok_ref[...].astype(F32)
    normed = (normalize(local) * gain_ref[...]).astype(BF)
    for j in range(8):
        nb[j] = normed[:, j * BLK : (j + 1) * BLK]
    pl.semaphore_wait(barrier, 33)

    for r, s in plane:
        send(nb.at[peers[r]], ga.at[r * 4 + q], pa_send, pa_recv, plane_dev[r, s])
    ga[q] = nb[dp]
    wait(ga.at[0:31], pa_recv)

    for r in range(8):
        unit = jnp.concatenate([ga[r * 4 + s].astype(F32) for s in range(4)], axis=0)
        xb[0, r * 16 : (r + 1) * 16, :] = unit.astype(BF)

    def ring_out(slot, to, h):
        rows = pl.ds(h * 64, 64)
        send(xb.at[slot, rows], xb.at[to, rows], zg_send, zg_recv.at[to // 2 * 2 + h], dev_up)

    for h in range(2):
        ring_out(0, 1, h)

    def ring_step(step):
        if step < 4:
            slot = 2 * step - 1
            for h in range(2):
                rows = pl.ds(h * 64, 64)
                wait(xb.at[slot, rows], zg_recv.at[slot // 2 * 2 + h])
                if step < 3:
                    ring_out(slot, slot + 2, h)
                send(xb.at[slot, rows], xb.at[slot + 1, rows], dg_send, dg_recv.at[slot // 2 * 2 + h], dev_pair)
            if step == 3:
                rows = pl.ds(half, 64)
                send(xb.at[slot, rows], xb.at[7, rows], zg_send, zg_recv.at[6], dev_up)
        else:
            rows = pl.ds(half, 64)
            wait(xb.at[7, rows], zg_recv.at[6])
            send(xb.at[7, rows], xb.at[7, rows], dg_send, dg_recv.at[6], dev_pair)

    def pair_step(step):
        if step < 4:
            slot = 2 * step
            for h in range(2):
                rows = pl.ds(h * 64, 64)
                wait(xb.at[slot, rows], dg_recv.at[(slot - 1) // 2 * 2 + h])
        else:
            wait(xb.at[7, pl.ds(other, 64)], dg_recv.at[6])

    cube = [tuple(peers[1 << d] for d in ROT[p]) for p in range(3)]

    def project(c):
        lo, hi = CHUNKS[c]
        rows = (hi - lo) * 128
        left = xb[lo:hi].reshape(rows, BLK)
        for p in range(3):
            res = jnp.dot(left, w1[:, p * 384 : (p + 1) * 384], preferred_element_type=F32)
            for k in range(lo, hi):
                for r in range(8):
                    at = (k - lo) * 128 + r * 16
                    u = first_unit(p, r)
                    if u >= 4:
                        s1[p, k, u - 4] = res[at : at + 16].astype(BF)
                    else:
                        k1[p, k, u] = res[at : at + 16]
            send(s1.at[p, lo:hi], r1.at[p, lo:hi], rs_send.at[0], rs_recv.at[c, p, 0], (cube[p][0], mp))

    def halve_1(c):
        lo, hi = CHUNKS[c]
        for p in range(3):
            wait(r1.at[p, lo:hi], rs_recv.at[c, p, 0])
            s2[p, lo:hi] = (k1[p, lo:hi, 2:4] + r1[p, lo:hi, 2:4].astype(F32)).astype(BF)
            send(s2.at[p, lo:hi], r2.at[p, lo:hi], rs_send.at[1], rs_recv.at[c, p, 1], (cube[p][1], mp))
            k2[p, lo:hi] = k1[p, lo:hi, 0:2] + r1[p, lo:hi, 0:2].astype(F32)

    def halve_2(c):
        lo, hi = CHUNKS[c]
        for p in range(3):
            wait(r2.at[p, lo:hi], rs_recv.at[c, p, 1])
            s3[p, lo:hi] = (k2[p, lo:hi, 1] + r2[p, lo:hi, 1].astype(F32)).astype(BF)
            send(s3.at[p, lo:hi], r3.at[p, lo:hi], rs_send.at[2], rs_recv.at[c, p, 2], (cube[p][2], mp))
            k3[p, lo:hi] = k2[p, lo:hi, 0] + r2[p, lo:hi, 0].astype(F32)

    def halve_3(c):
        lo, hi = CHUNKS[c]
        for p in range(3):
            wait(r3.at[p, lo:hi], rs_recv.at[c, p, 2])
            yb[p, lo:hi] = k3[p, lo:hi] + r3[p, lo:hi].astype(F32)

    for load in loads[:4]:
        load.wait()
    for t in range(8):
        if 1 <= t < 5:
            ring_step(t)
        if 0 <= t - 1 < 5:
            halve_1(t - 1)
        if 0 <= t - 2 < 5:
            halve_2(t - 2)
        if 0 <= t - 3 < 5:
            halve_3(t - 3)
        if t < 5:
            if t:
                pair_step(t)
            project(t)

    def put(ref, lo, hi, value):
        for k in range(8):
            ref[k, 0, :, lo:hi] = value[k * 16 : (k + 1) * 16]

    def activation(p, lo, hi):
        inner = yb[p].reshape(128, 384)[:, lo:hi] + bias_ref[:, (p - 1) * 384 + lo : (p - 1) * 384 + hi]
        return (0.5 * inner * (1.0 + lax.erf(inner * math.sqrt(0.5)))).astype(BF)

    put(g0, 128, 384, activation(1, 0, 256))
    put(g1, 0, 128, activation(1, 256, 384))
    put(g1, 128, 256, activation(2, 0, 128))
    put(g2, 0, 256, activation(2, 128, 384))

    heads = yb[0].reshape(128, 384)
    query = normalize(heads[:, 0:128].astype(BF).astype(F32)).astype(BF)
    keys = normalize(heads[:, 128:256].astype(BF).astype(F32)).astype(BF)
    values = heads[:, 256:384].astype(BF)
    scores = lax.dot_general(query, keys, (((1,), (1,)), ((), ())), preferred_element_type=F32)
    scores = scores * (temper_ref[...] / math.sqrt(HEAD))
    scores = jnp.exp(scores - jnp.max(scores, axis=-1, keepdims=True))
    probs = (scores / jnp.sum(scores, axis=-1, keepdims=True)).astype(BF)
    mixed = jnp.dot(probs, values, preferred_element_type=F32).astype(BF)
    put(g0, 0, 128, mixed)

    gs = (g0, g1, g2)
    back = CHUNKS[::-1]

    def double(c, stage):
        lo, hi = back[c]
        n = 1 << stage
        for p in range(3):
            if stage:
                m = n // 2
                wait(gs[p].at[lo:hi, m:n], ag_recv.at[c, p, stage - 1])
            send(
                gs[p].at[lo:hi, 0:n], gs[p].at[lo:hi, n : 2 * n],
                ag_send.at[p], ag_recv.at[c, p, stage], (cube[p][stage], mp),
            )

    def combine(c):
        lo, hi = back[c]
        for p in range(3):
            wait(gs[p].at[lo:hi, 4:8], ag_recv.at[c, p, 2])
            c0, c1 = GCOLS[p]
            for k in range(lo, hi):
                for r in range(8):
                    xa[k, r * 16 : (r + 1) * 16, c0:c1] = gs[p][k, last_unit(p, r)]
        left = xa[lo:hi].reshape((hi - lo) * 128, 896)
        for n in range(2):
            res = jnp.dot(left, w2[:, n * 384 : (n + 1) * 384], preferred_element_type=F32)
            tb[lo:hi, :, n * 384 : (n + 1) * 384] = res.reshape(hi - lo, 128, 384)
        if c == 0:
            d2s[3, 0:64] = tb[7, pl.ds(other, 64)].astype(BF)
            send(d2s.at[3, 0:64], d2r.at[3, 0:64], dr_send, dr_recv.at[3], dev_pair)
        elif c < 4:
            s = 4 - c
            d2s[s - 1] = tb[hi - 1].astype(BF)
            send(d2s.at[s - 1], d2r.at[s - 1], dr_send, dr_recv.at[s - 1], dev_pair)

    def ring_sum(c):
        if c == 0:
            wait(d2r.at[3, 0:64], dr_recv.at[3])
            zs[3, 0:64] = (tb[7, pl.ds(half, 64)] + d2r[3, 0:64].astype(F32)).astype(BF)
            send(zs.at[3, 0:64], zr.at[3, 0:64], zr_send, zr_recv.at[6], dev_down)
        elif c < 4:
            s = 4 - c
            lo, _ = back[c]
            wait(d2r.at[s - 1], dr_recv.at[s - 1])
            if c == 1:
                tb[lo] = tb[lo] + d2r[s - 1].astype(F32)
                wait(zr.at[3, 0:64], zr_recv.at[6])
                tb[lo, pl.ds(half, 64)] = tb[lo, pl.ds(half, 64)] + zr[3, 0:64].astype(F32)
            for h in range(2):
                rows = slice(h * 64, h * 64 + 64)
                part = tb[lo, rows]
                if c > 1:
                    wait(zr.at[s, rows], zr_recv.at[s * 2 + h])
                    part = part + d2r[s - 1, rows].astype(F32) + zr[s, rows].astype(F32)
                zs[s - 1, rows] = part.astype(BF)
                send(zs.at[s - 1, rows], zr.at[s - 1, rows], zr_send, zr_recv.at[(s - 1) * 2 + h], dev_down)
        else:
            for h in range(2):
                rows = slice(h * 64, h * 64 + 64)
                wait(zr.at[0, rows], zr_recv.at[h])
                part = tb[0, rows] + zr[0, rows].astype(F32)
                for r in range(4 * h, 4 * h + 4):
                    for s in range(4):
                        at = (r - 4 * h) * 16 + s * 4
                        fb[r * 4 + s] = part[at : at + 4].astype(BF)
                for r, s in plane:
                    if r // 4 == h:
                        send(
                            fb.at[r * 4 + (q + s) % 4], fr.at[r * 4 + q], pf_send, pf_recv, plane_dev[r, s]
                        )

    for t in range(8):
        if t < 5:
            double(t, 0)
        if 0 <= t - 1 < 5:
            double(t - 1, 1)
        if 0 <= t - 2 < 5:
            double(t - 2, 2)
        if 0 <= t - 3 < 5:
            if t == 3:
                for load in loads[4:]:
                    load.wait()
            combine(t - 3)
            ring_sum(t - 3)

    fr[q] = fb[q]
    wait(fr.at[0:31], pf_recv)
    for r in range(8):
        total = fr[r * 4].astype(F32)
        for s in range(1, 4):
            total = total + fr[r * 4 + s].astype(F32)
        cols = pl.ds(pl.multiple_of(peers[r] * BLK, BLK), BLK)
        out_ref[:, cols] = (tok_ref[:, cols].astype(F32) + total).astype(BF)

    wait(ga.at[0:31], pa_send)
    wait(xb.at[0:7, 0:64], zg_send)
    wait(xb.at[0:7, 0:64], dg_send)
    wait(s1, rs_send.at[0])
    wait(s2, rs_send.at[1])
    wait(s3, rs_send.at[2])
    for p in range(3):
        wait(gs[p].at[:, 0:7], ag_send.at[p])
    wait(d2s.at[:, 0:112], dr_send)
    wait(zs.at[:, 0:112], zr_send)
    wait(fb.at[0:31], pf_send)


def per_device(tokens, gain, w_query, w_key, w_value, w_inner, bias, w_attn_out, w_outer, temper):
    vmem = pl.BlockSpec(memory_space=pltpu.VMEM)
    anyw = pl.BlockSpec(memory_space=pl.ANY)
    dma = pltpu.SemaphoreType.DMA
    return pl.pallas_call(
        kernel,
        out_shape=jax.ShapeDtypeStruct(tokens.shape, BF),
        in_specs=[vmem, vmem, anyw, anyw, anyw, anyw, vmem, anyw, anyw, vmem],
        out_specs=vmem,
        scratch_shapes=[
            pltpu.VMEM((768, 1152), BF),
            pltpu.VMEM((896, 768), BF),
            pltpu.VMEM((8, 4, BLK), BF),
            pltpu.VMEM((32, 4, BLK), BF),
            pltpu.VMEM((8, 128, BLK), BF),
            pltpu.VMEM((3, 8, 4, 16, 384), BF),
            pltpu.VMEM((3, 8, 4, 16, 384), BF),
            pltpu.VMEM((3, 8, 4, 16, 384), F32),
            pltpu.VMEM((3, 8, 2, 16, 384), BF),
            pltpu.VMEM((3, 8, 2, 16, 384), BF),
            pltpu.VMEM((3, 8, 2, 16, 384), F32),
            pltpu.VMEM((3, 8, 16, 384), BF),
            pltpu.VMEM((3, 8, 16, 384), BF),
            pltpu.VMEM((3, 8, 16, 384), F32),
            pltpu.VMEM((3, 8, 16, 384), F32),
            pltpu.VMEM((8, 8, 16, 384), BF),
            pltpu.VMEM((8, 8, 16, 256), BF),
            pltpu.VMEM((8, 8, 16, 256), BF),
            pltpu.VMEM((8, 128, 896), BF),
            pltpu.VMEM((8, 128, BLK), F32),
            pltpu.VMEM((4, 128, BLK), BF),
            pltpu.VMEM((4, 128, BLK), BF),
            pltpu.VMEM((4, 128, BLK), BF),
            pltpu.VMEM((4, 128, BLK), BF),
            pltpu.VMEM((32, 4, BLK), BF),
            pltpu.VMEM((32, 4, BLK), BF),
            dma((6,)),
            dma, dma,
            dma, dma((7,)),
            dma, dma((7,)),
            dma((3,)), dma((5, 3, 3)),
            dma((3,)), dma((5, 3, 3)),
            dma, dma((4,)),
            dma, dma((7,)),
            dma, dma,
        ],
        compiler_params=pltpu.CompilerParams(
            collective_id=0, has_side_effects=True, vmem_limit_bytes=60 * 1024 * 1024
        ),
    )(
        tokens, gain.reshape(1, -1), w_query, w_key, w_value, w_inner, bias.reshape(1, -1),
        w_attn_out, w_outer, temper.reshape(1, 1),
    )


def solution(mesh):
    return jax.shard_map(
        per_device,
        mesh=mesh,
        in_specs=(
            P(("dp", "mp"), None),
            P(),
            P("dp", "mp"),
            P("dp", "mp"),
            P("dp", "mp"),
            P("dp", "mp"),
            P("mp"),
            P("mp", "dp"),
            P("mp", "dp"),
            P("mp"),
        ),
        out_specs=P(("dp", "mp"), None),
        check_vma=False,
    )
```

```python
import math

import jax
import jax.numpy as jnp
from jax import lax
from jax.experimental import pallas as pl
from jax.experimental.pallas import tpu as pltpu
from jax.sharding import PartitionSpec as P

BF = jnp.bfloat16
F32 = jnp.float32
MESH = pl.DeviceIdType.MESH
HEAD = 128
BLK = 768
ROT = ((2, 1, 0), (1, 0, 2), (0, 2, 1))
CHUNKS = ((0, 1), (1, 3), (3, 5), (5, 7), (7, 8))
GCOLS = ((0, 384), (384, 640), (640, 896))


def first_unit(part, r):
    a, b, c = ROT[part]
    return ((r >> a) & 1) * 4 + ((r >> b) & 1) * 2 + ((r >> c) & 1)


def last_unit(part, r):
    a, b, c = ROT[part]
    return ((r >> a) & 1) + ((r >> b) & 1) * 2 + ((r >> c) & 1) * 4


def normalize(values):
    center = values - jnp.mean(values, axis=-1, keepdims=True)
    spread = jnp.mean(center * center, axis=-1, keepdims=True)
    return center * lax.rsqrt(spread + 1e-06)


def kernel(
    tok_ref, gain_ref, wq_ref, wk_ref, wv_ref, wi_ref, bias_ref, wa_ref, wo_ref, temper_ref,
    out_ref,
    w1, w2, nb, ga, xb,
    s1, r1, k1, s2, r2, k2, s3, r3, k3, yb,
    g0, g1, g2, xa, tb, d2s, d2r, zs, zr, fb, fr,
    wsem, pa_send, pa_recv, zg_send, zg_recv, dg_send, dg_recv,
    rs_send, rs_recv, ag_send, ag_recv, dr_send, dr_recv, zr_send, zr_recv, pf_send, pf_recv,
):
    dp = lax.axis_index("dp")
    mp = lax.axis_index("mp")
    xl, y = dp // 4, dp % 4
    z, q, core = mp // 4, mp % 4, mp % 2

    def near(r):
        ys = (y, y + 1 - 2 * (y % 2), 3 - y, (y + 2) % 4)[r % 4]
        return (1 - xl if r >= 4 else xl) * 4 + ys

    peers = [near(r) for r in range(8)]
    up = (z + 1 - 2 * core + 8) % 8
    down = (z - 1 + 2 * core + 8) % 8
    dev_up = (dp, up * 4 + q)
    dev_down = (dp, down * 4 + q)
    dev_pair = (dp, mp + 1 - 2 * core)
    half = pl.multiple_of(core * 64, 64)
    other = pl.multiple_of(64 - core * 64, 64)

    def send(src, dst, ssem, rsem, dev):
        pltpu.make_async_remote_copy(
            src_ref=src, dst_ref=dst, send_sem=ssem, recv_sem=rsem, device_id=dev, device_id_type=MESH
        ).start()

    def wait(ref, sem):
        pltpu.make_async_copy(ref, ref, sem).wait()

    loads = [
        pltpu.make_async_copy(wq_ref, w1.at[:, 0:128], wsem.at[0]),
        pltpu.make_async_copy(wk_ref, w1.at[:, 128:256], wsem.at[1]),
        pltpu.make_async_copy(wv_ref, w1.at[:, 256:384], wsem.at[2]),
        pltpu.make_async_copy(wi_ref, w1.at[:, 384:1152], wsem.at[3]),
        pltpu.make_async_copy(wa_ref, w2.at[0:128], wsem.at[4]),
        pltpu.make_async_copy(wo_ref, w2.at[128:896], wsem.at[5]),
    ]
    for load in loads:
        load.start()

    plane = [(r, s) for r in range(8) for s in range(4) if (r, s) != (0, 0)]
    plane_dev = {(r, s): (peers[r], z * 4 + (q + s) % 4) for r, s in plane}

    barrier = pltpu.get_barrier_semaphore()
    for key in plane:
        pl.semaphore_signal(barrier, inc=1, device_id=plane_dev[key], device_id_type=MESH)
    for dev in (dev_up, dev_down):
        pl.semaphore_signal(barrier, inc=1, device_id=dev, device_id_type=MESH)

    def exchange():
        local = tok_ref[...].astype(F32)
        normed = (normalize(local) * gain_ref[...]).astype(BF)
        for j in range(8):
            nb[j] = normed[:, j * BLK : (j + 1) * BLK]
        with jax.named_scope('barrier'):
            pl.semaphore_wait(barrier, 33)

        for r, s in plane:
            send(nb.at[peers[r]], ga.at[r * 4 + q], pa_send, pa_recv, plane_dev[r, s])
        ga[q] = nb[dp]
        wait(ga.at[0:31], pa_recv)

        for r in range(8):
            unit = jnp.concatenate([ga[r * 4 + s].astype(F32) for s in range(4)], axis=0)
            xb[0, r * 16 : (r + 1) * 16, :] = unit.astype(BF)

    exchange()

    def ring_out(slot, to, h):
        rows = pl.ds(h * 64, 64)
        send(xb.at[slot, rows], xb.at[to, rows], zg_send, zg_recv.at[to // 2 * 2 + h], dev_up)

    for h in range(2):
        ring_out(0, 1, h)

    def ring_step(step):
        if step < 4:
            slot = 2 * step - 1
            for h in range(2):
                rows = pl.ds(h * 64, 64)
                wait(xb.at[slot, rows], zg_recv.at[slot // 2 * 2 + h])
                if step < 3:
                    ring_out(slot, slot + 2, h)
                send(xb.at[slot, rows], xb.at[slot + 1, rows], dg_send, dg_recv.at[slot // 2 * 2 + h], dev_pair)
            if step == 3:
                rows = pl.ds(half, 64)
                send(xb.at[slot, rows], xb.at[7, rows], zg_send, zg_recv.at[6], dev_up)
        else:
            rows = pl.ds(half, 64)
            wait(xb.at[7, rows], zg_recv.at[6])
            send(xb.at[7, rows], xb.at[7, rows], dg_send, dg_recv.at[6], dev_pair)

    def pair_step(step):
        if step < 4:
            slot = 2 * step
            for h in range(2):
                rows = pl.ds(h * 64, 64)
                wait(xb.at[slot, rows], dg_recv.at[(slot - 1) // 2 * 2 + h])
        else:
            wait(xb.at[7, pl.ds(other, 64)], dg_recv.at[6])

    cube = [tuple(peers[1 << d] for d in ROT[p]) for p in range(3)]

    def project(c):
        lo, hi = CHUNKS[c]
        rows = (hi - lo) * 128
        left = xb[lo:hi].reshape(rows, BLK)
        for p in range(3):
            res = jnp.dot(left, w1[:, p * 384 : (p + 1) * 384], preferred_element_type=F32)
            for k in range(lo, hi):
                for r in range(8):
                    at = (k - lo) * 128 + r * 16
                    u = first_unit(p, r)
                    if u >= 4:
                        s1[p, k, u - 4] = res[at : at + 16].astype(BF)
                    else:
                        k1[p, k, u] = res[at : at + 16]
            send(s1.at[p, lo:hi], r1.at[p, lo:hi], rs_send.at[0], rs_recv.at[c, p, 0], (cube[p][0], mp))

    def halve_1(c):
        lo, hi = CHUNKS[c]
        for p in range(3):
            wait(r1.at[p, lo:hi], rs_recv.at[c, p, 0])
            s2[p, lo:hi] = (k1[p, lo:hi, 2:4] + r1[p, lo:hi, 2:4].astype(F32)).astype(BF)
            send(s2.at[p, lo:hi], r2.at[p, lo:hi], rs_send.at[1], rs_recv.at[c, p, 1], (cube[p][1], mp))
            k2[p, lo:hi] = k1[p, lo:hi, 0:2] + r1[p, lo:hi, 0:2].astype(F32)

    def halve_2(c):
        lo, hi = CHUNKS[c]
        for p in range(3):
            wait(r2.at[p, lo:hi], rs_recv.at[c, p, 1])
            s3[p, lo:hi] = (k2[p, lo:hi, 1] + r2[p, lo:hi, 1].astype(F32)).astype(BF)
            send(s3.at[p, lo:hi], r3.at[p, lo:hi], rs_send.at[2], rs_recv.at[c, p, 2], (cube[p][2], mp))
            k3[p, lo:hi] = k2[p, lo:hi, 0] + r2[p, lo:hi, 0].astype(F32)

    def halve_3(c):
        lo, hi = CHUNKS[c]
        for p in range(3):
            wait(r3.at[p, lo:hi], rs_recv.at[c, p, 2])
            yb[p, lo:hi] = k3[p, lo:hi] + r3[p, lo:hi].astype(F32)

    for load in loads[:4]:
        load.wait()
    for t in range(8):
        if 1 <= t < 5:
            ring_step(t)
            pair_step(t)
        if t < 5:
            project(t)
        if 0 <= t - 1 < 5:
            halve_1(t - 1)
        if 0 <= t - 2 < 5:
            halve_2(t - 2)
        if 0 <= t - 3 < 5:
            halve_3(t - 3)

    def attend():
        def put(ref, lo, hi, value):
            for k in range(8):
                ref[k, 0, :, lo:hi] = value[k * 16 : (k + 1) * 16]

        def activation(p, lo, hi):
            inner = yb[p].reshape(128, 384)[:, lo:hi] + bias_ref[(p - 1) * 384 + lo : (p - 1) * 384 + hi].reshape(1, hi - lo)
            return (0.5 * inner * (1.0 + lax.erf(inner * math.sqrt(0.5)))).astype(BF)

        put(g0, 128, 384, activation(1, 0, 256))
        put(g1, 0, 128, activation(1, 256, 384))
        put(g1, 128, 256, activation(2, 0, 128))
        put(g2, 0, 256, activation(2, 128, 384))

        heads = yb[0].reshape(128, 384)
        query = normalize(heads[:, 0:128].astype(BF).astype(F32)).astype(BF)
        keys = normalize(heads[:, 128:256].astype(BF).astype(F32)).astype(BF)
        values = heads[:, 256:384].astype(BF)
        scores = lax.dot_general(query, keys, (((1,), (1,)), ((), ())), preferred_element_type=F32)
        scores = scores * (temper_ref[...] / math.sqrt(HEAD))
        scores = jnp.exp(scores - jnp.max(scores, axis=-1, keepdims=True))
        probs = (scores / jnp.sum(scores, axis=-1, keepdims=True)).astype(BF)
        mixed = jnp.dot(probs, values, preferred_element_type=F32).astype(BF)
        put(g0, 0, 128, mixed)


    attend()

    gs = (g0, g1, g2)
    back = CHUNKS[::-1]

    def double(c, stage):
        lo, hi = back[c]
        n = 1 << stage
        for p in range(3):
            if stage:
                m = n // 2
                wait(gs[p].at[lo:hi, m:n], ag_recv.at[c, p, stage - 1])
            send(
                gs[p].at[lo:hi, 0:n], gs[p].at[lo:hi, n : 2 * n],
                ag_send.at[p], ag_recv.at[c, p, stage], (cube[p][stage], mp),
            )

    def combine(c):
        lo, hi = back[c]
        for p in range(3):
            wait(gs[p].at[lo:hi, 4:8], ag_recv.at[c, p, 2])
            c0, c1 = GCOLS[p]
            for k in range(lo, hi):
                for r in range(8):
                    xa[k, r * 16 : (r + 1) * 16, c0:c1] = gs[p][k, last_unit(p, r)]
        left = xa[lo:hi].reshape((hi - lo) * 128, 896)
        for n in range(2):
            res = jnp.dot(left, w2[:, n * 384 : (n + 1) * 384], preferred_element_type=F32)
            tb[lo:hi, :, n * 384 : (n + 1) * 384] = res.reshape(hi - lo, 128, 384)
        if c == 0:
            d2s[3, 0:64] = tb[7, pl.ds(other, 64)].astype(BF)
            send(d2s.at[3, 0:64], d2r.at[3, 0:64], dr_send, dr_recv.at[3], dev_pair)
        elif c < 4:
            s = 4 - c
            d2s[s - 1] = tb[hi - 1].astype(BF)
            send(d2s.at[s - 1], d2r.at[s - 1], dr_send, dr_recv.at[s - 1], dev_pair)

    def ring_sum(c):
        if c == 0:
            wait(d2r.at[3, 0:64], dr_recv.at[3])
            zs[3, 0:64] = (tb[7, pl.ds(half, 64)] + d2r[3, 0:64].astype(F32)).astype(BF)
            send(zs.at[3, 0:64], zr.at[3, 0:64], zr_send, zr_recv.at[6], dev_down)
        elif c < 4:
            s = 4 - c
            lo, _ = back[c]
            wait(d2r.at[s - 1], dr_recv.at[s - 1])
            if c == 1:
                tb[lo] = tb[lo] + d2r[s - 1].astype(F32)
                wait(zr.at[3, 0:64], zr_recv.at[6])
                tb[lo, pl.ds(half, 64)] = tb[lo, pl.ds(half, 64)] + zr[3, 0:64].astype(F32)
            for h in range(2):
                rows = slice(h * 64, h * 64 + 64)
                part = tb[lo, rows]
                if c > 1:
                    wait(zr.at[s, rows], zr_recv.at[s * 2 + h])
                    part = part + d2r[s - 1, rows].astype(F32) + zr[s, rows].astype(F32)
                zs[s - 1, rows] = part.astype(BF)
                send(zs.at[s - 1, rows], zr.at[s - 1, rows], zr_send, zr_recv.at[(s - 1) * 2 + h], dev_down)
        else:
            for h in range(2):
                rows = slice(h * 64, h * 64 + 64)
                wait(zr.at[0, rows], zr_recv.at[h])
                part = tb[0, rows] + zr[0, rows].astype(F32)
                for r in range(4 * h, 4 * h + 4):
                    for s in range(4):
                        at = (r - 4 * h) * 16 + s * 4
                        fb[r * 4 + s] = part[at : at + 4].astype(BF)
                for r, s in plane:
                    if r // 4 == h:
                        send(
                            fb.at[r * 4 + (q + s) % 4], fr.at[r * 4 + q], pf_send, pf_recv, plane_dev[r, s]
                        )

    for t in range(5):
        double(t, 0)
    for t in range(7):
        if t < 5:
            double(t, 1)
        if 0 <= t - 1 < 5:
            double(t - 1, 2)
        if 0 <= t - 2 < 5:
            if t == 2:
                for load in loads[4:]:
                    load.wait()
            combine(t - 2)
            ring_sum(t - 2)

    def finish():
        fr[q] = fb[q]
        wait(fr.at[0:31], pf_recv)
        for r in range(8):
            total = fr[r * 4].astype(F32)
            for s in range(1, 4):
                total = total + fr[r * 4 + s].astype(F32)
            cols = pl.ds(pl.multiple_of(peers[r] * BLK, BLK), BLK)
            out_ref[:, cols] = (tok_ref[:, cols].astype(F32) + total).astype(BF)


    finish()

    def drain():
        wait(ga.at[0:31], pa_send)
        wait(xb.at[0:7, 0:64], zg_send)
        wait(xb.at[0:7, 0:64], dg_send)
        wait(s1, rs_send.at[0])
        wait(s2, rs_send.at[1])
        wait(s3, rs_send.at[2])
        for p in range(3):
            wait(gs[p].at[:, 0:7], ag_send.at[p])
        wait(d2s.at[:, 0:112], dr_send)
        wait(zs.at[:, 0:112], zr_send)
        wait(fb.at[0:31], pf_send)

    drain()


def per_device(tokens, gain, w_query, w_key, w_value, w_inner, bias, w_attn_out, w_outer, temper):
    vmem = pl.BlockSpec(memory_space=pltpu.VMEM)
    anyw = pl.BlockSpec(memory_space=pl.ANY)
    dma = pltpu.SemaphoreType.DMA
    return pl.pallas_call(
        kernel,
        out_shape=jax.ShapeDtypeStruct(tokens.shape, BF),
        in_specs=[vmem, vmem, anyw, anyw, anyw, anyw, vmem, anyw, anyw, vmem],
        out_specs=vmem,
        scratch_shapes=[
            pltpu.VMEM((768, 1152), BF),
            pltpu.VMEM((896, 768), BF),
            pltpu.VMEM((8, 4, BLK), BF),
            pltpu.VMEM((32, 4, BLK), BF),
            pltpu.VMEM((8, 128, BLK), BF),
            pltpu.VMEM((3, 8, 4, 16, 384), BF),
            pltpu.VMEM((3, 8, 4, 16, 384), BF),
            pltpu.VMEM((3, 8, 4, 16, 384), F32),
            pltpu.VMEM((3, 8, 2, 16, 384), BF),
            pltpu.VMEM((3, 8, 2, 16, 384), BF),
            pltpu.VMEM((3, 8, 2, 16, 384), F32),
            pltpu.VMEM((3, 8, 16, 384), BF),
            pltpu.VMEM((3, 8, 16, 384), BF),
            pltpu.VMEM((3, 8, 16, 384), F32),
            pltpu.VMEM((3, 8, 16, 384), F32),
            pltpu.VMEM((8, 8, 16, 384), BF),
            pltpu.VMEM((8, 8, 16, 256), BF),
            pltpu.VMEM((8, 8, 16, 256), BF),
            pltpu.VMEM((8, 128, 896), BF),
            pltpu.VMEM((8, 128, BLK), F32),
            pltpu.VMEM((4, 128, BLK), BF),
            pltpu.VMEM((4, 128, BLK), BF),
            pltpu.VMEM((4, 128, BLK), BF),
            pltpu.VMEM((4, 128, BLK), BF),
            pltpu.VMEM((32, 4, BLK), BF),
            pltpu.VMEM((32, 4, BLK), BF),
            dma((6,)),
            dma, dma,
            dma, dma((7,)),
            dma, dma((7,)),
            dma((3,)), dma((5, 3, 3)),
            dma((3,)), dma((5, 3, 3)),
            dma, dma((4,)),
            dma, dma((7,)),
            dma, dma,
        ],
        compiler_params=pltpu.CompilerParams(
            collective_id=0, has_side_effects=True, vmem_limit_bytes=60 * 1024 * 1024
        ),
    )(
        tokens, gain.reshape(1, -1), w_query, w_key, w_value, w_inner, bias,
        w_attn_out, w_outer, temper.reshape(1, 1),
    )


def solution(mesh):
    return jax.shard_map(
        per_device,
        mesh=mesh,
        in_specs=(
            P(("dp", "mp"), None),
            P(),
            P("dp", "mp"),
            P("dp", "mp"),
            P("dp", "mp"),
            P("dp", "mp"),
            P("mp"),
            P("mp", "dp"),
            P("mp", "dp"),
            P("mp"),
        ),
        out_specs=P(("dp", "mp"), None),
        check_vma=False,
    )
```
